256 devices in a mesh: space: 8 (over y_hi, x), exc: 32 (over z, y_lo, core).
Axes of the slice: x: 4, y: 4 (y_hi: 2, y_lo: 2; y = y_hi * 2 + y_lo), z: 8, core: 2. Of those that a mesh axis runs over, the one named last changes fastest.
Arguments:
- coeff: float32 [64, 256, 16384], P('space', None, 'exc'), may hold values from -6 to 6
- factors: float32 [4, 64, 256, 512], P(None, 'space', 'exc'), may hold values from -0.25 to 0.25
Outputs:
- applied: float32 [64, 256, 16384], P('space', None, 'exc')
The draws below stay inside these ranges and needn't reach their ends.
All inputs are finite; a program needn't handle non-finite values.
Results may differ from the reference program's by a relative error of at most 0.0003.
Values sent between devices are 32-bit elements; how exact they have to be, the bound alone decides.
No kernel may reach another device: no remote copies, remote signals or barrier semaphores. Data moves between devices by JAX's collectives and lax.ppermute only.
A program may use at most 128 MiB of HBM per device.

```python
import jax
import jax.numpy as jnp
from jax import lax

BLOCKS = 64
BITS = 6
RANK = 256
LEVELS = 4
EXC = 16384


def levels(key, extent, pieces, low, top_value):
    factor_of, own = 1.0, jax.random.fold_in(key, 6)
    for axis_at, blocks in pieces:
        draws = jnp.exp(jax.random.uniform(jax.random.fold_in(own, axis_at), (blocks,), jnp.float32, low / len(pieces), top_value / len(pieces)))
        factor_of = factor_of * jnp.repeat(draws, extent[axis_at] // blocks).reshape([-1 if axis == axis_at else 1 for axis in range(len(extent))])
    return factor_of


def scatter_about(key, dims, deviation, bound, cuts=(), kind=jnp.bfloat16):
    loudness = levels(key, dims, cuts, -0.22, 0.18) if cuts else 1.0
    drawn = jax.random.normal(key, dims, jnp.float32) * deviation * loudness
    return jnp.minimum(jnp.maximum(drawn, -bound), bound).astype(kind)


def setup_inputs(seed: int = 0) -> dict:
    streams_of = jax.random.split(jax.random.key(seed), 3)
    coeff = scatter_about(streams_of[0], (BLOCKS, RANK, EXC), 1.0, 6.0, ((0, 8), (2, 32)), jnp.float32)
    factors = scatter_about(streams_of[1], (LEVELS, BLOCKS, RANK, 2 * RANK), (2 * RANK) ** -0.5, 0.25, ((1, 8), (2, 32)), jnp.float32)
    return {"coeff": coeff, "factors": factors}


def apply_level(state, level_factors, stride):
    def one_block(index):
        upper = (index // stride) % 2
        partner = (index + stride - 2 * stride * upper).astype(jnp.int32)
        stacked = jnp.concatenate([state[index], state[partner]], axis=0)
        return jnp.dot(level_factors[index], stacked, precision=lax.Precision.HIGHEST, preferred_element_type=jnp.float32)
    return lax.map(one_block, jnp.arange(BLOCKS, dtype=jnp.int32))


def reference(coeff, factors):
    state = coeff
    for level in range(LEVELS):
        stride = 2 ** (BITS - LEVELS + level)
        state = apply_level(state, factors[level], stride)
    return state
```

```python
import jax
import jax.numpy as jnp
from jax import lax
from jax.experimental import pallas as pl
from jax.experimental.pallas import tpu as pltpu
from jax.sharding import Mesh, PartitionSpec as P


def split(value):
    high = value.astype(jnp.bfloat16)
    return high, (value - high.astype(jnp.float32)).astype(jnp.bfloat16)


def product(left, right):
    def dot(a, b):
        return jnp.dot(a, b, preferred_element_type=jnp.float32)

    return dot(left[0], right[0]) + (dot(left[0], right[1]) + dot(left[1], right[0]))


def level_kernel(rows_ref, state_ref, out_ref):
    lower = split(state_ref[0, 0, 0])
    upper = split(state_ref[0, 1, 0])
    sides, short = rows_ref.shape[0], 8
    for half in range(2):
        pieces = []
        for z in range(8):
            for side in range(sides):
                for core in range(2):
                    start = (z * 2 + core) * short
                    pieces.append(rows_ref[side, 0, half, 0, 0, start : start + short, :])
        rows = jnp.concatenate(pieces, axis=0)
        rank = rows.shape[1] // 2
        own, other = (lower, upper) if half == 0 else (upper, lower)
        out_ref[0, half, 0] = product(split(rows[:, :rank]), own) + product(split(rows[:, rank:]), other)


def apply_level(rows, level, state, stride):
    count, rank, columns = state.shape
    outer = count // (2 * stride)
    sides, _, levels, tall, wide = rows.shape
    rows = rows.reshape(sides, outer, 2, stride, levels, tall, wide)
    state = state.reshape(outer, 2, stride, rank, columns)
    spec = pl.BlockSpec((1, 2, 1, rank, columns), lambda p: (p // stride, 0, p % stride, 0, 0))
    out = pl.pallas_call(
        level_kernel,
        grid=(count // 2,),
        in_specs=[
            pl.BlockSpec(
                (sides, 1, 2, 1, 1, tall, wide), lambda p: (0, p // stride, 0, p % stride, level, 0, 0)
            ),
            spec,
        ],
        out_specs=spec,
        out_shape=jax.ShapeDtypeStruct(state.shape, jnp.float32),
        compiler_params=pltpu.CompilerParams(dimension_semantics=("arbitrary",), vmem_limit_bytes=40 << 20),
        cost_estimate=pl.CostEstimate(
            flops=6 * count * rank * wide * columns,
            transcendentals=0,
            bytes_accessed=4 * count * rank * (wide + 2 * columns),
        ),
    )(rows, state)
    return out.reshape(count, rank, columns)


def gather(shard):
    partner = lax.ppermute(shard, "yl", [(0, 1), (1, 0)])
    upper = lax.axis_index("yl") == 1
    both = jnp.stack([jnp.where(upper, partner, shard), jnp.where(upper, shard, partner)])
    return lax.all_gather(both, ("z", "core"), axis=3, tiled=True)


def body(coeff, factors):
    space = ("yh", "x")
    factors = jnp.swapaxes(factors, 0, 1)
    first = gather(factors[:, :1])
    rest = gather(lax.all_to_all(factors[:, 1:], space, split_axis=0, concat_axis=0, tiled=True))
    state = apply_level(first, 0, coeff, 4)
    state = lax.all_to_all(state, space, split_axis=0, concat_axis=0, tiled=True)
    for level in range(3):
        state = apply_level(rest, level, state, 1 << level)
    return lax.all_to_all(state, space, split_axis=0, concat_axis=0, tiled=True)


def solution(mesh):
    fine = Mesh(mesh.devices.reshape(2, 4, 8, 2, 2), ("yh", "x", "z", "yl", "core"))
    space, exc = ("yh", "x"), ("z", "yl", "core")
    return jax.shard_map(
        body,
        mesh=fine,
        in_specs=(P(space, None, exc), P(None, space, exc, None)),
        out_specs=P(space, None, exc),
        check_vma=False,
    )
```

```python
import jax
import jax.numpy as jnp
from jax import lax
from jax.experimental import pallas as pl
from jax.experimental.pallas import tpu as pltpu
from jax.sharding import Mesh, PartitionSpec as P

SHORT = 8
PLACES = 8
GROUP = 1


def split(value):
    high = value.astype(jnp.bfloat16)
    return high, (value - high.astype(jnp.float32)).astype(jnp.bfloat16)


def in_hbm(value):
    return pltpu.with_memory_space_constraint(value, pltpu.HBM)


def block_of(step, member, count, strides):
    steps = count // (2 * GROUP)
    level, pair = step // steps, step % steps * GROUP + member // 2
    found = 0
    for index, stride in enumerate(strides):
        block = (pair // stride) * 2 * stride + pair % stride + member % 2 * stride
        found = jnp.where(level == index, block, found)
    return found


def apply_levels(rows, here, state, strides):
    count, rank, columns = state.shape
    sides, _, _, tall, wide = rows[0].shape
    levels, last, members = len(strides), strides[-1], 2 * GROUP
    steps = count // members

    def kernel(here_ref, *refs):
        taken_refs = [refs[index * members : (index + 1) * members] for index in range(len(rows))]
        state_refs = refs[len(rows) * members : (len(rows) + 1) * members]
        (out_ref,) = refs[(len(rows) + 1) * members :]
        step = pl.program_id(0)
        blocks = [block_of(step, member, count, strides) for member in range(members)]
        if levels > 1:

            @pl.when(step < steps)
            def _():
                for member in range(members):
                    out_ref[blocks[member]] = state_refs[member][0]

        def row_of(member, place, side, core):
            index = side ^ here_ref[0]
            if len(rows) == 1:
                start = (place * 2 + core) * SHORT
                return taken_refs[0][member][index, 0, 0, start : start + SHORT, :]
            start = place * SHORT
            both = [refs[member][index, 0, 0, start : start + SHORT, :] for refs in taken_refs]
            return jnp.where(here_ref[1] == core, both[0], both[1])

        def rows_of(member):
            parts = []
            for place in range(PLACES):
                for side in range(2):
                    for core in range(2):
                        parts.append((place, side, core))
            return jnp.concatenate([row_of(member, *part) for part in parts], axis=0)

        results = []
        for pair in range(GROUP):
            two = (2 * pair, 2 * pair + 1)
            if levels > 1:
                state_rows = [out_ref[blocks[member]] for member in two]
            else:
                state_rows = [state_refs[member][0] for member in two]
            high, low = split(jnp.concatenate(state_rows, axis=0))
            lower, upper = (rows_of(member) for member in two)
            upper = jnp.concatenate([upper[:, rank:], upper[:, :rank]], axis=1)
            rows_high, rows_low = split(jnp.concatenate([lower, upper], axis=0))
            result = jnp.dot(
                jnp.concatenate([rows_high, rows_high, rows_low], axis=1),
                jnp.concatenate([high, low, high], axis=0),
                preferred_element_type=jnp.float32,
            )
            results.append(result)

        for member in range(members):
            at = member % 2 * rank
            value = results[member // 2][at : at + rank]
            if levels == 1:
                out_ref[0, member % 2, member // 2] = value
            else:
                out_ref[blocks[member]] = value

    def rows_spec(member):
        return pl.BlockSpec(
            (sides, 1, 1, tall, wide),
            lambda s, here_ref: (0, block_of(s, member, count, strides), s // steps, 0, 0),
        )

    def state_spec(member):
        return pl.BlockSpec(
            (1, rank, columns),
            lambda s, here_ref: (block_of(jnp.minimum(s, steps - 1), member, count, strides), 0, 0),
        )

    if levels == 1:
        out_block, out_index = (1, 2, GROUP, rank, columns), lambda s, here_ref: (0, 0, s, 0, 0)
        out_shape = (1, 2, last, rank, columns)
    else:
        out_block, out_index = state.shape, lambda s, here_ref: (0, 0, 0)
        out_shape = state.shape
    assert 2 * last == count
    rows, state = [in_hbm(rows[0]), *rows[1:]], in_hbm(state)
    out = pl.pallas_call(
        kernel,
        grid_spec=pltpu.PrefetchScalarGridSpec(
            num_scalar_prefetch=1,
            grid=(levels * steps,),
            in_specs=[rows_spec(member) for _ in rows for member in range(members)]
            + [state_spec(member) for member in range(members)],
            out_specs=pl.BlockSpec(out_block, out_index),
        ),
        out_shape=jax.ShapeDtypeStruct(out_shape, jnp.float32),
        compiler_params=pltpu.CompilerParams(dimension_semantics=("arbitrary",), vmem_limit_bytes=36 << 20),
        cost_estimate=pl.CostEstimate(
            flops=6 * levels * count * rank * wide * columns,
            transcendentals=0,
            bytes_accessed=4 * count * rank * (levels * wide + 2 * columns),
        ),
    )(here, *[value for value in rows for _ in range(members)], *[state] * members)
    return out.reshape(count, rank, columns)


def swap(value, axis):
    return lax.ppermute(value, axis, [(0, 1), (1, 0)])


def sides_of(shard):
    return jnp.stack([shard, swap(shard, "yl")])


def body(coeff, factors):
    space = ("yh", "x")
    side, core = (lax.axis_index(name).astype(jnp.int32) for name in ("yl", "core"))
    own = lax.all_gather(sides_of(factors[0][:, None]), "z", axis=3, tiled=True)
    other = swap(own, "core")
    later = jnp.swapaxes(factors[1:], 0, 1)
    later = sides_of(lax.all_to_all(later, space, split_axis=0, concat_axis=0, tiled=True))
    rest = lax.all_gather(later, ("z", "core"), axis=3, tiled=True)
    here = jnp.stack([side, core])
    state = apply_levels([own, other], here, coeff, (4,))
    state = lax.all_to_all(state, space, split_axis=0, concat_axis=0, tiled=True)
    state = apply_levels([rest], here, state, (1, 2, 4))
    return lax.all_to_all(state, space, split_axis=0, concat_axis=0, tiled=True)


def solution(mesh):
    fine = Mesh(mesh.devices.reshape(2, 4, 8, 2, 2), ("yh", "x", "z", "yl", "core"))
    space, exc = ("yh", "x"), ("z", "yl", "core")
    return jax.shard_map(
        body,
        mesh=fine,
        in_specs=(P(space, None, exc), P(None, space, exc, None)),
        out_specs=P(space, None, exc),
        check_vma=False,
    )
```

```python
import jax
import jax.numpy as jnp
from jax import lax
from jax.experimental import pallas as pl
from jax.experimental.pallas import tpu as pltpu
from jax.sharding import Mesh, PartitionSpec as P

SHORT = 8
PLACES = 8
GROUP = 1


def split(value):
    high = value.astype(jnp.bfloat16)
    return high, (value - high.astype(jnp.float32)).astype(jnp.bfloat16)


def in_hbm(value):
    return pltpu.with_memory_space_constraint(value, pltpu.HBM)


def block_of(step, member, count, strides):
    steps = count // (2 * GROUP)
    level, pair = step // steps, step % steps * GROUP + member // 2
    found = 0
    for index, stride in enumerate(strides):
        block = (pair // stride) * 2 * stride + pair % stride + member % 2 * stride
        found = jnp.where(level == index, block, found)
    return found


def apply_levels(rows, here, state, strides):
    count, rank, columns = state.shape
    sides, _, _, tall, wide = rows[0].shape
    levels, last, members = len(strides), strides[-1], 2 * GROUP
    steps = count // members

    def kernel(here_ref, *refs):
        taken_refs = [refs[index * members : (index + 1) * members] for index in range(len(rows))]
        state_refs = refs[len(rows) * members : (len(rows) + 1) * members]
        out_ref, left_ref, right_ref = refs[(len(rows) + 1) * members :]
        step = pl.program_id(0)
        blocks = [block_of(step, member, count, strides) for member in range(members)]
        if levels > 1:

            @pl.when(step < steps)
            def _():
                for member in range(members):
                    out_ref[blocks[member]] = state_refs[member][0]

        def rows_of(member, place, side):
            index = side ^ here_ref[0]
            if len(rows) == 1:
                start = place * 2 * SHORT
                return taken_refs[0][member][index, 0, 0, start : start + 2 * SHORT, :]
            start = place * SHORT
            own, other = [refs[member][index, 0, 0, start : start + SHORT, :] for refs in taken_refs]
            first = here_ref[1] == 0
            return jnp.concatenate([jnp.where(first, own, other), jnp.where(first, other, own)], axis=0)

        for member in range(2):
            for place in range(PLACES):
                for side in range(2):
                    high, low = split(rows_of(member, place, side))
                    start = member * rank + (place * 2 + side) * 2 * SHORT
                    where = slice(start, start + 2 * SHORT)
                    for third, value in enumerate((high, high, low)):
                        for half in range(2):
                            at = third * wide + (half ^ member) * rank
                            left_ref[where, at : at + rank] = value[:, half * rank : (half + 1) * rank]
            for start in range(0, rank, 32):
                if levels > 1:
                    value = out_ref[blocks[member], start : start + 32, :]
                else:
                    value = state_refs[member][0, start : start + 32, :]
                high, low = split(value)
                for third, value in enumerate((high, low, high)):
                    at = third * wide + member * rank + start
                    right_ref[at : at + 32, :] = value
        results = [jnp.dot(left_ref[...], right_ref[...], preferred_element_type=jnp.float32)]

        for member in range(members):
            at = member % 2 * rank
            value = results[member // 2][at : at + rank]
            if levels == 1:
                out_ref[0, member % 2, member // 2] = value
            else:
                out_ref[blocks[member]] = value

    def rows_spec(member):
        return pl.BlockSpec(
            (sides, 1, 1, tall, wide),
            lambda s, here_ref: (0, block_of(s, member, count, strides), s // steps, 0, 0),
        )

    def state_spec(member):
        return pl.BlockSpec(
            (1, rank, columns),
            lambda s, here_ref: (block_of(jnp.minimum(s, steps - 1), member, count, strides), 0, 0),
        )

    if levels == 1:
        out_block, out_index = (1, 2, GROUP, rank, columns), lambda s, here_ref: (0, 0, s, 0, 0)
        out_shape = (1, 2, last, rank, columns)
    else:
        out_block, out_index = state.shape, lambda s, here_ref: (0, 0, 0)
        out_shape = state.shape
    assert 2 * last == count
    rows, state = [in_hbm(rows[0]), *rows[1:]], in_hbm(state)
    out = pl.pallas_call(
        kernel,
        grid_spec=pltpu.PrefetchScalarGridSpec(
            num_scalar_prefetch=1,
            grid=(levels * steps,),
            in_specs=[rows_spec(member) for _ in rows for member in range(members)]
            + [state_spec(member) for member in range(members)],
            out_specs=pl.BlockSpec(out_block, out_index),
            scratch_shapes=[
                pltpu.VMEM((2 * rank, 3 * wide), jnp.bfloat16),
                pltpu.VMEM((3 * wide, columns), jnp.bfloat16),
            ],
        ),
        out_shape=jax.ShapeDtypeStruct(out_shape, jnp.float32),
        compiler_params=pltpu.CompilerParams(dimension_semantics=("arbitrary",), vmem_limit_bytes=36 << 20),
        cost_estimate=pl.CostEstimate(
            flops=6 * levels * count * rank * wide * columns,
            transcendentals=0,
            bytes_accessed=4 * count * rank * (levels * wide + 2 * columns),
        ),
    )(here, *[value for value in rows for _ in range(members)], *[state] * members)
    return out.reshape(count, rank, columns)


def apply_rest(rows, here, state, strides):
    count, rank, columns = state.shape
    sides, _, _, tall, wide = rows.shape
    steps = count // 2
    total = len(strides) * steps

    def kernel(here_ref, *refs):
        row_refs, (state_ref, out_ref, left_a, left_b, right_a, right_b) = refs[:6], refs[6:]
        turn = pl.program_id(0)

        def ready_left(left_ref, two):
            for member in range(2):
                for place in range(PLACES):
                    for side in range(2):
                        begin = place * 2 * SHORT
                        high, low = split(two[member][side ^ here_ref[0], 0, 0, begin : begin + 2 * SHORT, :])
                        start = member * rank + (place * 2 + side) * 2 * SHORT
                        for third, value in enumerate((high, high, low)):
                            for half in range(2):
                                at = third * wide + (half ^ member) * rank
                                left_ref[start : start + 2 * SHORT, at : at + rank] = value[
                                    :, half * rank : (half + 1) * rank
                                ]

        def ready_right(right_ref, blocks):
            for member in range(2):
                for start in range(0, rank, 32):
                    high, low = split(out_ref[blocks[member], start : start + 32, :])
                    for third, value in enumerate((high, low, high)):
                        at = third * wide + member * rank + start
                        right_ref[at : at + 32, :] = value

        @pl.when(turn == 0)
        def _():
            ready_left(left_a, row_refs[:2])

        @pl.when(turn < 2)
        def _():
            out_ref[pl.ds(turn * 4, 4)] = state_ref[...]

        for part in range(2):
            left_ref, right_ref, next_ref = ((left_a, right_a, left_b), (left_b, right_b, left_a))[part]
            blocks = [block_of(2 * turn + part, member, count, strides) for member in range(2)]
            ready_right(right_ref, blocks)
            result = jnp.dot(left_ref[...], right_ref[...], preferred_element_type=jnp.float32)
            ready_left(next_ref, row_refs[2 + 2 * part : 4 + 2 * part])
            for member in range(2):
                out_ref[blocks[member]] = result[member * rank : (member + 1) * rank]

    def rows_spec(ahead, member):
        def index(turn, here_ref):
            step = 0 * turn if ahead == 0 else jnp.minimum(2 * turn + ahead, total - 1)
            return 0, block_of(step, member, count, strides), step // steps, 0, 0

        return pl.BlockSpec((sides, 1, 1, tall, wide), index)

    assert strides[0] == 1 and count == 8 and GROUP == 1
    rows, state = in_hbm(rows), in_hbm(state)
    return pl.pallas_call(
        kernel,
        grid_spec=pltpu.PrefetchScalarGridSpec(
            num_scalar_prefetch=1,
            grid=(total // 2,),
            in_specs=[rows_spec(ahead, member) for ahead in range(3) for member in range(2)]
            + [pl.BlockSpec((4, rank, columns), lambda turn, here_ref: (jnp.minimum(turn, 1), 0, 0))],
            out_specs=pl.BlockSpec(state.shape, lambda turn, here_ref: (0, 0, 0)),
            scratch_shapes=[pltpu.VMEM((2 * rank, 3 * wide), jnp.bfloat16)] * 2
            + [pltpu.VMEM((3 * wide, columns), jnp.bfloat16)] * 2,
        ),
        out_shape=jax.ShapeDtypeStruct(state.shape, jnp.float32),
        compiler_params=pltpu.CompilerParams(dimension_semantics=("arbitrary",), vmem_limit_bytes=44 << 20),
        cost_estimate=pl.CostEstimate(
            flops=6 * len(strides) * count * rank * wide * columns,
            transcendentals=0,
            bytes_accessed=4 * count * rank * (len(strides) * wide + 2 * columns),
        ),
    )(here, *[rows] * 6, state)


def swap(value, axis):
    return lax.ppermute(value, axis, [(0, 1), (1, 0)])


def sides_of(shard):
    return jnp.stack([shard, swap(shard, "yl")])


def body(coeff, factors):
    space = ("yh", "x")
    side, core = (lax.axis_index(name).astype(jnp.int32) for name in ("yl", "core"))
    own = lax.all_gather(sides_of(factors[0][:, None]), "z", axis=3, tiled=True)
    other = swap(own, "core")
    later = jnp.swapaxes(factors[1:], 0, 1)
    later = sides_of(lax.all_to_all(later, space, split_axis=0, concat_axis=0, tiled=True))
    rest = lax.all_gather(later, ("z", "core"), axis=3, tiled=True)
    here = jnp.stack([side, core])
    state = apply_levels([own, other], here, coeff, (4,))
    state = lax.all_to_all(state, space, split_axis=0, concat_axis=0, tiled=True)
    state = apply_rest(rest, here, state, (1, 2, 4))
    return lax.all_to_all(state, space, split_axis=0, concat_axis=0, tiled=True)


def solution(mesh):
    fine = Mesh(mesh.devices.reshape(2, 4, 8, 2, 2), ("yh", "x", "z", "yl", "core"))
    space, exc = ("yh", "x"), ("z", "yl", "core")
    return jax.shard_map(
        body,
        mesh=fine,
        in_specs=(P(space, None, exc), P(None, space, exc, None)),
        out_specs=P(space, None, exc),
        check_vma=False,
    )
```
